32 devices in a mesh: group: 2 (over y), ha: 4 (over x, core), wa: 4 (over z).
Axes of the slice: x: 2, y: 2, z: 4, core: 2. Of those that a mesh axis runs over, the one named last changes fastest.
Arguments:
- queries: bfloat16 [4, 32, 32, 1536], P('group', 'ha', 'wa'), parts along dimension 0, may hold values from -6 to 6
- keys: bfloat16 [4, 32, 32, 1536], P('group', 'ha', 'wa'), parts along dimension 0, may hold values from -6 to 6
- values: bfloat16 [4, 32, 32, 1536], P('group', 'ha', 'wa'), parts along dimension 0, may hold values from -6 to 6
- out_grad: bfloat16 [4, 32, 32, 1536], P('group', 'ha', 'wa'), parts along dimension 0, may hold values from -96 to 96
- log_norm: float32 [12, 4, 32, 32], P(None, 'group', 'ha', 'wa'), parts along dimension 1, may hold values from 6.5 to 7.5
- delta_rows: float32 [12, 4, 32, 32], P(None, 'group', 'ha', 'wa'), parts along dimension 1, may hold values from -360 to 360
- text_keys: bfloat16 [64, 1536], P('group'), parts along dimension 0, may hold values from -6 to 6
- text_values: bfloat16 [64, 1536], P('group'), parts along dimension 0, may hold values from -6 to 6
- window_table: int32 [4, 4, 9], replicated, may hold values 0 or 1
Outputs:
- query_grad: bfloat16 [4, 32, 32, 1536], P('group', 'ha', 'wa'), parts along dimension 0
- key_grad: bfloat16 [4, 32, 32, 1536], P('group', 'ha', 'wa'), parts along dimension 0
- value_grad: bfloat16 [4, 32, 32, 1536], P('group', 'ha', 'wa'), parts along dimension 0
- text_key_grad: bfloat16 [64, 1536], P('group'), parts along dimension 0
- text_value_grad: bfloat16 [64, 1536], P('group'), parts along dimension 0
The draws below stay inside these ranges and needn't reach their ends.
There are 2 independent parts, one for each index of `group`. The reference program is written for one: setup_inputs(seed, part) draws one part's arguments, and reference() takes and returns one part's arrays. A program takes and returns all parts, laid end to end along the dimension named above; an argument that names none is the same for every part. Nothing has to cross between parts.
All inputs are finite; a program needn't handle non-finite values.
Results may differ from the reference program's by a relative error of at most 0.001.
The reference program's roundings to bfloat16 on the way (of `probs_half` and `score_grad`) count: a program that leaves them out, or rounds other values in their place, can miss the bound.
Values may be sent and summed in bfloat16 or wider, within the bound.
A program may use at most 64 MiB of HBM per device.

```python
import jax
import jax.numpy as jnp
from jax import lax

HEADS = 12
HDIM = 128
TEXT = 32
FRAMES = 2
TILE = 8
HALO = 2
HD = 1536
NH = 32
NW = 32
N_HA = 4
N_WA = 4


def place_ends(array, own_key, least, high):
    place = [jax.random.randint(jax.random.fold_in(own_key, axis), (), 0, length) for axis, length in enumerate(array.shape)]
    longest = array.shape.index(max(array.shape))
    neighbour = place[:longest] + [(place[longest] + 1) % array.shape[longest]] + place[longest + 1:]
    return array.at[tuple(place)].set(least).at[tuple(neighbour)].set(high)


def shard_levels(stream_key, dims, split, least, largest):
    gain, own = 1.0, jax.random.fold_in(stream_key, 6)
    for axis_at, shards_of in split:
        heights = jnp.exp(jax.random.uniform(jax.random.fold_in(own, axis_at), (shards_of,), jnp.float32, least / len(split), largest / len(split)))
        gain = gain * jnp.repeat(heights, dims[axis_at] // shards_of).reshape([-1 if axis == axis_at else 1 for axis in range(len(dims))])
    return gain


def gaussian(rng, dims, scale, most, shards=(), kind=jnp.bfloat16):
    drawn = jax.random.normal(rng, dims, jnp.float32) * scale
    if len(shards) > 0:
        drawn = shard_levels(rng, dims, shards, -0.22, 0.18) * drawn
    return jnp.clip(drawn, min=-most, max=most).astype(kind)


def setup_inputs(seed: int = 0, part: int = 0) -> dict:
    streams_of = jax.random.split(jax.random.key(seed), 10)
    part_keys = jax.random.split(jax.random.fold_in(streams_of[9], part), 10)
    return {
        "queries": gaussian(part_keys[0], (FRAMES, NH, NW, HD), 1.0, 6.0, ((1, 4), (2, 4))),
        "keys": gaussian(part_keys[1], (FRAMES, NH, NW, HD), 1.0, 6.0, ((1, 4), (2, 4))),
        "values": gaussian(part_keys[2], (FRAMES, NH, NW, HD), 1.0, 6.0, ((1, 4), (2, 4))),
        "out_grad": gaussian(part_keys[3], (FRAMES, NH, NW, HD), 16.0, 96.0, ((1, 4), (2, 4))),
        "log_norm": jnp.clip(6.5 + 1.0 * jax.random.uniform(part_keys[4], (HEADS, FRAMES, NH, NW), jnp.float32) ** shard_levels(part_keys[4], (HEADS, FRAMES, NH, NW), ((2, 4), (3, 4)), -0.2, 0.2), 6.5, 7.5),
        "delta_rows": gaussian(part_keys[5], (HEADS, FRAMES, NH, NW), 60.0, 360.0, ((2, 4), (3, 4)), jnp.float32),
        "text_keys": gaussian(part_keys[6], (TEXT, HD), 1.0, 6.0),
        "text_values": gaussian(part_keys[7], (TEXT, HD), 1.0, 6.0),
        "window_table": place_ends((jax.random.randint(streams_of[8], (N_HA, N_WA, 9), 0, 4) < 3).astype(jnp.int32), jax.random.fold_in(streams_of[8], 1), 0, 1),
    }


def tile_grads(query_rows, cotangent_rows, norm_rows, delta_part, key_rows, value_rows, cell_mask):
    score_scale = 1.0 / (HDIM ** 0.5)
    query_wide = query_rows.astype(jnp.float32)
    cotangent_wide = cotangent_rows.astype(jnp.float32)
    key_wide = key_rows.astype(jnp.float32)
    value_wide = value_rows.astype(jnp.float32)
    scores = jnp.einsum("qhd,khd->hqk", query_wide, key_wide) * score_scale
    probs = jnp.exp(scores - norm_rows[:, :, None])
    if cell_mask is not None:
        probs = probs * cell_mask[None, None, :]
    probs_half = probs.astype(jnp.bfloat16)
    value_part = jnp.einsum("hqk,qhd->khd", probs_half.astype(jnp.float32), cotangent_wide)
    prob_grad = jnp.einsum("qhd,khd->hqk", cotangent_wide, value_wide)
    score_grad = (probs * (prob_grad - delta_part[:, :, None])).astype(jnp.bfloat16).astype(jnp.float32)
    query_part = jnp.einsum("hqk,khd->qhd", score_grad, key_wide) * score_scale
    key_part = jnp.einsum("hqk,qhd->khd", score_grad, query_wide) * score_scale
    return query_part, key_part, value_part


def reference(queries, keys, values, out_grad, log_norm, delta_rows, text_keys, text_values, window_table):
    frames, rows_all, cols_all, width = queries.shape
    tile_side = TILE
    halo_rim = HALO
    window_side = TILE + 2 * HALO
    pad_spec = ((0, 0), (halo_rim, halo_rim), (halo_rim, halo_rim), (0, 0))
    key_pad = jnp.pad(keys, pad_spec, mode="wrap")
    value_pad = jnp.pad(values, pad_spec, mode="wrap")
    position = jnp.arange(window_side, dtype=jnp.int32)
    block_of = (position >= halo_rim).astype(jnp.int32) + (position >= halo_rim + tile_side).astype(jnp.int32)
    text_key_rows = text_keys.reshape(TEXT, HEADS, HDIM)
    text_value_rows = text_values.reshape(TEXT, HEADS, HDIM)

    def per_tile(carry, tile_index):
        grad_pad, text_total = carry
        row_tile = (tile_index // N_WA).astype(jnp.int32)
        col_tile = (tile_index % N_WA).astype(jnp.int32)
        row_start = (row_tile * tile_side).astype(jnp.int32)
        col_start = (col_tile * tile_side).astype(jnp.int32)
        anchor = jnp.zeros((), jnp.int32)
        tile_shape = (frames, tile_side, tile_side, width)
        query_rows = lax.dynamic_slice(queries, (anchor, row_start, col_start, anchor), tile_shape).reshape(-1, HEADS, HDIM)
        cotangent_rows = lax.dynamic_slice(out_grad, (anchor, row_start, col_start, anchor), tile_shape).reshape(-1, HEADS, HDIM)
        stat_shape = (HEADS, frames, tile_side, tile_side)
        norm_rows = lax.dynamic_slice(log_norm, (anchor, anchor, row_start, col_start), stat_shape).reshape(HEADS, -1)
        delta_part = lax.dynamic_slice(delta_rows, (anchor, anchor, row_start, col_start), stat_shape).reshape(HEADS, -1)
        window_shape = (frames, window_side, window_side, width)
        key_rows = lax.dynamic_slice(key_pad, (anchor, row_start, col_start, anchor), window_shape).reshape(-1, HEADS, HDIM)
        value_rows = lax.dynamic_slice(value_pad, (anchor, row_start, col_start, anchor), window_shape).reshape(-1, HEADS, HDIM)
        pattern = lax.dynamic_slice(window_table, (row_tile, col_tile, anchor), (1, 1, 9)).reshape(9).astype(jnp.float32)
        cell_grid = pattern[3 * block_of[:, None] + block_of[None, :]]
        cell_mask = jnp.broadcast_to(cell_grid[None], (frames, window_side, window_side)).reshape(-1)
        video_query, video_key, video_value = tile_grads(query_rows, cotangent_rows, norm_rows, delta_part, key_rows, value_rows, cell_mask)
        text_query, text_key, text_value = tile_grads(query_rows, cotangent_rows, norm_rows, delta_part, text_key_rows, text_value_rows, None)
        query_tile = (video_query + text_query).astype(jnp.bfloat16).reshape(tile_shape)
        window_grad = jnp.stack((video_key, video_value)).reshape((2,) + window_shape)
        start = (anchor, anchor, row_start, col_start, anchor)
        current = lax.dynamic_slice(grad_pad, start, window_grad.shape)
        grad_pad = lax.dynamic_update_slice(grad_pad, current + window_grad, start)
        text_total = text_total + jnp.stack((text_key, text_value))
        return (grad_pad, text_total), query_tile

    grad_start = jnp.zeros((2, frames, rows_all + 2 * halo_rim, cols_all + 2 * halo_rim, width), jnp.float32)
    text_start = jnp.zeros((2, TEXT, HEADS, HDIM), jnp.float32)
    (grad_pad, text_total), query_tiles = lax.scan(per_tile, (grad_start, text_start), jnp.arange(N_HA * N_WA, dtype=jnp.int32))
    folded = grad_pad[:, :, halo_rim:halo_rim + rows_all]
    folded = folded.at[:, :, :halo_rim].add(grad_pad[:, :, halo_rim + rows_all:])
    folded = folded.at[:, :, rows_all - halo_rim:].add(grad_pad[:, :, :halo_rim])
    core = folded[:, :, :, halo_rim:halo_rim + cols_all]
    core = core.at[:, :, :, :halo_rim].add(folded[:, :, :, halo_rim + cols_all:])
    core = core.at[:, :, :, cols_all - halo_rim:].add(folded[:, :, :, :halo_rim])
    query_grad = query_tiles.reshape(N_HA, N_WA, frames, tile_side, tile_side, width)
    query_grad = query_grad.transpose(2, 0, 3, 1, 4, 5).reshape(frames, rows_all, cols_all, width)
    text_key_grad = text_total[0].reshape(TEXT, HEADS * HDIM).astype(jnp.bfloat16)
    text_value_grad = text_total[1].reshape(TEXT, HEADS * HDIM).astype(jnp.bfloat16)
    return query_grad, core[0].astype(jnp.bfloat16), core[1].astype(jnp.bfloat16), text_key_grad, text_value_grad
```

```python
import functools
import math

import jax
import jax.numpy as jnp
from jax import lax
from jax.experimental import pallas as pl
from jax.experimental.pallas import tpu as pltpu
from jax.sharding import PartitionSpec as P

HDIM = 128
HALO = 2
GROUPS = 4
MESH = pl.DeviceIdType.MESH
F32 = jnp.float32
BF16 = jnp.bfloat16
I16 = jnp.int16
STEPS = 32766.0
LEAST = 1e-30
LOG2E = math.log2(math.e)


def text_plan(n_ha, n_wa, blocks, width):
    plan = []

    def halve(axis, count):
        nonlocal blocks, width
        far = 1
        while far < count:
            if blocks > 1:
                blocks //= 2
                plan.append((axis, far, blocks, width, "rows"))
            elif width % 256 == 0:
                width //= 2
                plan.append((axis, far, blocks, width, "cols"))
            else:
                plan.append((axis, far, blocks, width, "none"))
            far *= 2

    halve("ha", n_ha)
    if width % (n_wa * 128) == 0:
        plan.append(("wa", n_wa, blocks, width // n_wa, "direct"))
    else:
        halve("wa", n_wa)
    return plan


def contract(a, b, dims):
    return lax.dot_general(a, b, (dims, ((), ())), preferred_element_type=F32)


def encode(x):
    most = jnp.maximum(jnp.max(jnp.abs(x), axis=0, keepdims=True), LEAST)
    codes = jnp.round(x * (STEPS / most)).astype(jnp.int32).astype(I16)
    return codes, most * (1.0 / STEPS)


def decode(codes, steps):
    return codes.astype(jnp.int32).astype(F32) * steps


def kernel(n_ha, n_wa, plan, *refs):
    (table_h, q_h, k_h, v_h, g_h, norm_h, delta_h, tk_h, tv_h) = refs[:9]
    (dq_ref, dk_ref, dv_ref, dtk_ref, dtv_ref) = refs[9:14]
    (
        table, q_ref, k_ref, v_ref, g_ref, norm_ref, delta_ref, tk_ref, tv_ref,
        stage, hcol, hrow, hcor, part_col,
        out_col, out_row, out_cor, in_col, in_row, in_cor,
        st_col, st_row, st_cor, sr_col, sr_row, sr_cor,
        own, dq_acc, mask, norm, delta, tx, tb,
    ) = refs[14:47]
    trecv = refs[47:47 + len(plan)]
    (
        load_s, col_s, col_r, row_s, row_r, cor_s, cor_r,
        mid_s, mid_r, rr_s, rr_r, rq_s, rq_r, end_s, end_r,
        t_s, t_r, u_s, u_r,
    ) = refs[47 + len(plan):]

    frames, plane, width = q_ref.shape
    tile = math.isqrt(plane)
    cells = frames * plane
    text = tk_ref.shape[0]
    heads = width // HDIM
    part = width // GROUPS
    per = heads // GROUPS
    bands = tile // HALO
    band = frames * HALO * HALO
    strip = bands * band
    rim = frames * HALO * tile
    scale = 1.0 / math.sqrt(HDIM)
    ha, wa = lax.axis_index("ha"), lax.axis_index("wa")
    ha_of = [{"ha": lax.rem(ha + n_ha - 1, n_ha)}, {"ha": lax.rem(ha + 1, n_ha)}]
    wa_of = [{"wa": lax.rem(wa + n_wa - 1, n_wa)}, {"wa": lax.rem(wa + 1, n_wa)}]

    partners, bits = [], []
    for axis, far, _, _, how in plan:
        at = ha if axis == "ha" else wa
        if how == "direct":
            bits.append(None)
            partners.append([{axis: lax.rem(at + hop, far)} for hop in range(1, far)])
        else:
            bit = lax.rem(lax.div(at, far), 2)
            bits.append(bit)
            partners.append([{axis: at + far * (1 - 2 * bit)}])

    barrier = pltpu.get_barrier_semaphore()
    greeted = ha_of + wa_of + sum(partners, [])
    for other in greeted:
        pl.semaphore_signal(barrier, inc=1, device_id=other, device_id_type=MESH)

    loads = []
    for n, (src, dst) in enumerate((
        (k_h, k_ref), (v_h, v_ref), (q_h, q_ref), (g_h, g_ref), (tk_h, tk_ref), (tv_h, tv_ref),
        (norm_h, norm_ref), (delta_h, delta_ref), (table_h, table),
    )):
        c = pltpu.make_async_copy(src, dst, load_s.at[n])
        c.start()
        loads.append(c)

    def cols(g):
        return slice(g * part, (g + 1) * part)

    def lanes(h):
        return slice(h * HDIM, (h + 1) * HDIM)

    def remote(src, dst, s, r, device):
        c = pltpu.make_async_remote_copy(
            src_ref=src, dst_ref=dst, send_sem=s, recv_sem=r, device_id=device, device_id_type=MESH
        )
        c.start()
        return c

    def cell_of(j):
        side = lax.div(j, strip)
        at_band = lax.rem(lax.div(j, band), bands)
        frame = lax.rem(lax.div(j, HALO * HALO), frames)
        row = at_band * HALO + lax.rem(lax.div(j, HALO), HALO)
        col = lax.rem(j, HALO) + side * (tile - HALO)
        return frame * plane + row * tile + col

    border = 2 * strip
    lane = lax.broadcasted_iota(jnp.int32, (border, cells), 1)
    pick = (lane == cell_of(lax.broadcasted_iota(jnp.int32, (border, cells), 0))).astype(F32).astype(BF16)
    back_row = lax.broadcasted_iota(jnp.int32, (cells, 2 * border), 0)
    back_lane = lax.broadcasted_iota(jnp.int32, (cells, 2 * border), 1)
    put_back = (back_row == cell_of(lax.rem(back_lane, border))).astype(F32).astype(BF16)

    def whole(ref, where):
        return ref[:, :, where].reshape(cells, where.stop - where.start)

    col_copy, row_copy, cor_copy, mid_copy, rr_copy, rq_copy, end_copy = {}, {}, {}, {}, {}, {}, {}

    def send_rows(g):
        for v in range(2):
            lo = v * (tile - HALO) * tile
            for kv, ref in enumerate((k_ref, v_ref)):
                row_copy[g, v, kv] = remote(
                    ref.at[:, lo:lo + HALO * tile, cols(g)], hrow.at[g, kv, 1 - v],
                    row_s.at[g, v, kv], row_r.at[g, 1 - v, kv], ha_of[v],
                )

    def pick_cols(g):
        for kv, ref in enumerate((k_ref, v_ref)):
            found = contract(pick, whole(ref, cols(g)), ((1,), (0,))).astype(BF16)
            for d in range(2):
                stage[g, kv, d] = found[d * strip:(d + 1) * strip]

    def send_cols(g):
        for d in range(2):
            col_copy[g, d] = remote(
                stage.at[g, :, d], hcol.at[g, :, 1 - d], col_s.at[g, d], col_r.at[g, 1 - d], wa_of[d]
            )

    loads[0].wait()
    loads[1].wait()
    pick_cols(0)
    pl.semaphore_wait(barrier, len(greeted))
    send_cols(0)
    send_rows(0)
    for g in range(1, GROUPS):
        pick_cols(g)
        send_cols(g)
        send_rows(g)

    for c in loads[2:]:
        c.wait()
    square = (cells, cells)
    same = (lax.broadcasted_iota(jnp.int32, square, 0) == lax.broadcasted_iota(jnp.int32, square, 1)).astype(F32)
    for src, dst, times in ((norm_ref, norm, LOG2E), (delta_ref, delta, 1.0)):
        dst[...] = times * lax.dot_general(
            src[...], same, (((0,), (0,)), ((), ())), precision=lax.Precision.HIGHEST, preferred_element_type=F32
        )

    def live(block):
        return table[ha, wa, block].astype(F32)

    at = 0
    for block, rows in ((1, rim), (7, rim), (0, band), (2, band), (6, band), (8, band), (3, strip), (5, strip)):
        mask[at:at + rows, :] = jnp.full((rows, cells), live(block), F32)
        at += rows
    own_live = live(4)

    def attend(todo, masking, sink):
        ahead = []

        def finish(h, keys, s, dp, qh, gh):
            p = masking(jnp.exp2(s * (scale * LOG2E) - norm[h:h + 1, :]))
            ds = (p * (dp - delta[h:h + 1, :])).astype(BF16)
            dv = contract(p.astype(BF16), gh, ((1,), (0,)))
            dk = contract(ds, qh, ((1,), (0,)))
            dq = contract(ds, keys, ((0,), (0,)))
            sink(h, dq, dk, dv)

        for h, keys, values in todo:
            qh, gh = whole(q_ref, lanes(h)), whole(g_ref, lanes(h))
            s = contract(keys, qh, ((1,), (1,)))
            dp = contract(values, gh, ((1,), (1,)))
            ahead.append((h, keys, s, dp, qh, gh))
            if len(ahead) > 1:
                finish(*ahead.pop(0))
        for left in ahead:
            finish(*left)

    def local(g):
        todo = []
        for h in range(g * per, (g + 1) * per):
            keys, values = (
                jnp.concatenate([whole(ref, lanes(h)), more[:, lanes(h)]], 0)
                for ref, more in ((k_ref, tk_ref), (v_ref, tv_ref))
            )
            todo.append((h, keys, values))

        def masking(p):
            return jnp.concatenate([p[:cells] * own_live, p[cells:]], 0)

        def sink(h, dq, dk, dv):
            here = lanes(h)
            dq_acc[:, here] = dq
            own[0, :, here] = dk[:cells]
            own[1, :, here] = dv[:cells]
            tx[: text // 8, :, here] = (dk[cells:] * scale).reshape(text // 8, 8, HDIM)
            tx[text // 8:, :, here] = dv[cells:].reshape(text // 8, 8, HDIM)

        attend(todo, masking, sink)

    def halo(g, rows_of, weights, sink):
        todo = []
        for n in range(per):
            keys, values = (rows_of(kv, lanes(n)) for kv in range(2))
            todo.append((g * per + n, keys, values))

        def take(h, dq, dk, dv):
            dq_acc[:, lanes(h)] += dq
            sink(lanes(h - g * per), (dk, dv))

        attend(todo, lambda p: p * weights, take)

    def forward(g):
        for d in range(2):
            col_copy[g, d].wait()
        for d in range(2):
            for v in range(2):
                lo = v * (strip - band)
                to = ((1 - v) * 2 + d) * band
                cor_copy[g, d, v] = remote(
                    hcol.at[g, :, d, lo:lo + band], hcor.at[g, :, to:to + band],
                    cor_s.at[g, d, v], cor_r.at[g, d, 1 - v], ha_of[v],
                )

    def columns(g):
        def sink(here, grads):
            for kv in range(2):
                for d in range(2):
                    lo = d * strip
                    codes, steps = encode(grads[kv][lo + band:lo + strip - band])
                    out_col[g, d, kv, band:strip - band, here] = codes
                    st_col[g, d, 1, kv:kv + 1, here] = steps
                    for v in range(2):
                        at = lo + v * (strip - band)
                        part_col[g, d, v, kv, :, here] = grads[kv][at:at + band]

        halo(
            g, lambda kv, here: hcol[g, kv, :, :, here].reshape(border, HDIM), mask[2 * rim + 4 * band:], sink
        )
        for d in range(2):
            mid_copy[g, d] = (
                remote(
                    out_col.at[g, d, :, band:strip - band], in_col.at[g, 1 - d, :, band:strip - band],
                    mid_s.at[g, d, 0], mid_r.at[g, 1 - d, 0], wa_of[d],
                ),
                remote(
                    st_col.at[g, d, 1], sr_col.at[g, 1 - d, 1], mid_s.at[g, d, 1], mid_r.at[g, 1 - d, 1], wa_of[d]
                ),
            )

    def strips(g):
        for v in range(2):
            for kv in range(2):
                row_copy[g, v, kv].wait()

        def sink(here, grads):
            for kv in range(2):
                for v in range(2):
                    codes, steps = encode(grads[kv][v * rim:(v + 1) * rim])
                    out_row[g, v, kv, :, here] = codes
                    st_row[g, v, kv:kv + 1, here] = steps

        halo(
            g, lambda kv, here: hrow[g, kv, :, :, :, here].reshape(2 * rim, HDIM), mask[:2 * rim], sink
        )
        for v in range(2):
            rr_copy[g, v] = (
                remote(out_row.at[g, v], in_row.at[g, 1 - v], rr_s.at[g, v, 0], rr_r.at[g, 1 - v, 0], ha_of[v]),
                remote(st_row.at[g, v], sr_row.at[g, 1 - v], rr_s.at[g, v, 1], rr_r.at[g, 1 - v, 1], ha_of[v]),
            )

    def corners(g):
        for v in range(2):
            for d in range(2):
                cor_copy[g, d, v].wait()

        def sink(here, grads):
            for kv in range(2):
                for v in range(2):
                    codes, steps = encode(grads[kv][2 * v * band:2 * (v + 1) * band])
                    out_cor[g, v, kv, :, here] = codes
                    st_cor[g, v, kv:kv + 1, here] = steps

        halo(g, lambda kv, here: hcor[g, kv, :, here], mask[2 * rim:2 * rim + 4 * band], sink)
        for v in range(2):
            rq_copy[g, v] = (
                remote(out_cor.at[g, v], in_cor.at[g, 1 - v], rq_s.at[g, v, 0], rq_r.at[g, 1 - v, 0], ha_of[v]),
                remote(st_cor.at[g, v], sr_cor.at[g, 1 - v], rq_s.at[g, v, 1], rq_r.at[g, 1 - v, 1], ha_of[v]),
            )

    def fold_corners(g):
        for v in range(2):
            for c in rq_copy[g, v]:
                c.wait()
        for v in range(2):
            for kv in range(2):
                came = decode(in_cor[g, v, kv], sr_cor[g, v, kv:kv + 1])
                for d in range(2):
                    total = part_col[g, d, v, kv] + came[d * band:(d + 1) * band]
                    codes, steps = encode(total)
                    at = v * (strip - band)
                    out_col[g, d, kv, at:at + band, :] = codes
                    st_col[g, d, 2 * v, kv:kv + 1, :] = steps
        for v in range(2):
            for d in range(2):
                at = v * (strip - band)
                end_copy[g, d, v] = (
                    remote(
                        out_col.at[g, d, :, at:at + band], in_col.at[g, 1 - d, :, at:at + band],
                        end_s.at[g, d, v, 0], end_r.at[g, 1 - d, v, 0], wa_of[d],
                    ),
                    remote(
                        st_col.at[g, d, 2 * v], sr_col.at[g, 1 - d, 2 * v],
                        end_s.at[g, d, v, 1], end_r.at[g, 1 - d, v, 1], wa_of[d],
                    ),
                )

    def fold_rows(g):
        for v in range(2):
            for c in rr_copy[g, v]:
                c.wait()
        for v in range(2):
            for kv in range(2):
                came = decode(in_row[g, v, kv], sr_row[g, v, kv:kv + 1])
                for f in range(frames):
                    lo = f * plane + v * (tile - HALO) * tile
                    own[kv, lo:lo + HALO * tile, cols(g)] += came[f * HALO * tile:(f + 1) * HALO * tile]

    def finish_queries(g):
        dq_ref[:, cols(g)] = (dq_acc[:, cols(g)] * scale).astype(BF16)

    def fold_cols(g):
        for d in range(2):
            for c in mid_copy[g, d] + end_copy[g, d, 0] + end_copy[g, d, 1]:
                c.wait()
        for kv, out in enumerate((dk_ref, dv_ref)):
            came = []
            for d in range(2):
                for piece, lo, hi in ((0, 0, band), (1, band, strip - band), (2, strip - band, strip)):
                    came.append(decode(in_col[g, d, kv, lo:hi], sr_col[g, d, piece, kv:kv + 1]))
            came = jnp.concatenate(came, 0)
            first = came.astype(BF16)
            second = (came - first.astype(F32)).astype(BF16)
            total = own[kv, :, cols(g)] + contract(put_back, jnp.concatenate([first, second], 0), ((1,), (0,)))
            if kv == 0:
                total = total * scale
            out[:, cols(g)] = total.astype(BF16)

    region = {"row": 0, "rows": 2 * text // 8, "col": 0, "cols": width}
    sums, regions = [], []

    def area(ref, row, rows, col, wide):
        where = pl.ds(pl.multiple_of(col, 128), wide) if not isinstance(col, int) else pl.ds(col, wide)
        return ref.at[pl.ds(row, rows), :, where]

    def mine(ref):
        return area(ref, region["row"], region["rows"], region["col"], region["cols"])

    def text_send(i):
        _, far, rows, wide, how = plan[i]
        regions.append(dict(region))
        row, col, bit = region["row"], region["col"], bits[i]
        if how == "direct":
            out = []
            for hop in range(1, far):
                to = lax.rem(wa + hop, far)
                out.append(remote(
                    area(tx, row, rows, col + to * wide, wide), trecv[i].at[hop - 1],
                    t_s.at[i, hop - 1], t_r.at[i, hop - 1], partners[i][hop - 1],
                ))
            region.update(col=col + wa * wide, cols=wide)
            sums.append(out)
            return
        send_row, send_col = row, col
        if how == "rows":
            send_row = row + (1 - bit) * rows
            region.update(row=row + bit * rows, rows=rows)
        elif how == "cols":
            send_col = col + (1 - bit) * wide
            region.update(col=col + bit * wide, cols=wide)
        sums.append([remote(
            area(tx, send_row, rows, send_col, wide), trecv[i].at[0], t_s.at[i, 0], t_r.at[i, 0], partners[i][0]
        )])

    def text_add(i):
        kept = mine(tx)
        for n, c in enumerate(sums[i]):
            c.wait()
        total = kept[...]
        for n in range(len(sums[i])):
            total = total + trecv[i][n]
        kept[...] = total

    gathers = []

    def text_spread(i):
        if i == len(plan) - 1:
            mine(tb)[...] = mine(tx)[...].astype(BF16)
        out = []
        if plan[i][4] != "none":
            for n, partner in enumerate(partners[i]):
                out.append(remote(mine(tb), mine(tb), u_s.at[i, n], u_r.at[i, n], partner))
        gathers.append(out)

    def text_join(i):
        for c in gathers.pop():
            c.wait()
        region.update(regions[i])

    steps = []
    for i in range(len(plan)):
        steps += [functools.partial(text_send, i), functools.partial(text_add, i)]
    for i in reversed(range(len(plan))):
        steps += [functools.partial(text_spread, i), functools.partial(text_join, i)]
    waiting = [steps[:1]] + [steps[n:n + 2] for n in range(1, len(steps) - 1, 2)] + [steps[-1:]]

    def text_step():
        if waiting:
            for step in waiting.pop(0):
                step()

    for g in range(GROUPS):
        local(g)
    text_step()
    strips(0)
    forward(0)
    columns(0)
    text_step()
    strips(1)
    forward(1)
    columns(1)
    corners(0)
    text_step()
    strips(2)
    forward(2)
    columns(2)
    fold_corners(0)
    corners(1)
    strips(3)
    forward(3)
    columns(3)
    text_step()
    fold_corners(1)
    corners(2)
    for g in range(GROUPS):
        fold_rows(g)
    fold_corners(2)
    corners(3)
    text_step()
    for g in range(GROUPS):
        finish_queries(g)
    fold_corners(3)
    while waiting:
        text_step()
    dtk_ref[...] = tb[: text // 8].astype(F32).reshape(text, width).astype(BF16)
    dtv_ref[...] = tb[text // 8:].astype(F32).reshape(text, width).astype(BF16)
    for g in range(GROUPS):
        fold_cols(g)


def hand_on(*refs):
    count = (len(refs) - 1) // 2
    copies = []
    for n in range(count):
        c = pltpu.make_async_copy(refs[n], refs[count + n], refs[-1].at[n])
        c.start()
        copies.append(c)
    for c in copies:
        c.wait()


def solution(mesh):
    n_ha, n_wa = mesh.shape["ha"], mesh.shape["wa"]

    def local(queries, keys, values, out_grad, log_norm, delta_rows, text_keys, text_values, window_table):
        frames, tile, _, width = queries.shape
        heads = width // HDIM
        text = text_keys.shape[0]
        plane = tile * tile
        cells = frames * plane
        part = width // GROUPS
        bands = tile // HALO
        band = frames * HALO * HALO
        strip = bands * band
        rim = frames * HALO * tile
        plan = text_plan(n_ha, n_wa, 2 * text // 8, width)
        most = max([far - 1 if how == "direct" else 1 for _, far, _, _, how in plan] + [1])
        received = []
        for _, far, rows, wide, how in plan:
            received.append(pltpu.VMEM((far - 1 if how == "direct" else 1, rows, 8, wide), F32))
        sem = pltpu.SemaphoreType.DMA
        anywhere = pl.BlockSpec(memory_space=pltpu.HBM)
        vmem = pl.BlockSpec(memory_space=pltpu.VMEM)
        rows = frames * plane
        results = pl.pallas_call(
            functools.partial(kernel, n_ha, n_wa, plan),
            out_shape=[pltpu.VMEM((rows, width), BF16)] * 3 + [pltpu.VMEM((text, width), BF16)] * 2,
            in_specs=[anywhere] * 9,
            out_specs=[vmem] * 5,
            scratch_shapes=[
                pltpu.SMEM(window_table.shape, jnp.int32),
                *[pltpu.VMEM((frames, plane, width), BF16)] * 4,
                *[pltpu.VMEM((cells, heads), F32)] * 2,
                *[pltpu.VMEM((text, width), BF16)] * 2,
                pltpu.VMEM((GROUPS, 2, 2, strip, part), BF16),
                pltpu.VMEM((GROUPS, 2, 2, strip, part), BF16),
                pltpu.VMEM((GROUPS, 2, 2, frames, HALO * tile, part), BF16),
                pltpu.VMEM((GROUPS, 2, 4 * band, part), BF16),
                pltpu.VMEM((GROUPS, 2, 2, 2, band, part), F32),
                pltpu.VMEM((GROUPS, 2, 2, strip, part), I16),
                pltpu.VMEM((GROUPS, 2, 2, rim, part), I16),
                pltpu.VMEM((GROUPS, 2, 2, 2 * band, part), I16),
                pltpu.VMEM((GROUPS, 2, 2, strip, part), I16),
                pltpu.VMEM((GROUPS, 2, 2, rim, part), I16),
                pltpu.VMEM((GROUPS, 2, 2, 2 * band, part), I16),
                pltpu.VMEM((GROUPS, 2, 3, 2, part), F32),
                pltpu.VMEM((GROUPS, 2, 2, part), F32),
                pltpu.VMEM((GROUPS, 2, 2, part), F32),
                pltpu.VMEM((GROUPS, 2, 3, 2, part), F32),
                pltpu.VMEM((GROUPS, 2, 2, part), F32),
                pltpu.VMEM((GROUPS, 2, 2, part), F32),
                pltpu.VMEM((2, cells, width), F32),
                pltpu.VMEM((cells, width), F32),
                pltpu.VMEM((2 * rim + 4 * band + 2 * strip, cells), F32),
                pltpu.VMEM((heads, cells), F32),
                pltpu.VMEM((heads, cells), F32),
                pltpu.VMEM((2 * text // 8, 8, width), F32),
                pltpu.VMEM((2 * text // 8, 8, width), BF16),
                *received,
                sem((9,)),
                sem((GROUPS, 2)), sem((GROUPS, 2)),
                sem((GROUPS, 2, 2)), sem((GROUPS, 2, 2)),
                sem((GROUPS, 2, 2)), sem((GROUPS, 2, 2)),
                sem((GROUPS, 2, 2)), sem((GROUPS, 2, 2)),
                sem((GROUPS, 2, 2)), sem((GROUPS, 2, 2)),
                sem((GROUPS, 2, 2)), sem((GROUPS, 2, 2)),
                sem((GROUPS, 2, 2, 2)), sem((GROUPS, 2, 2, 2)),
                sem((len(plan), most)), sem((len(plan), most)),
                sem((len(plan), most)), sem((len(plan), most)),
            ],
            compiler_params=pltpu.CompilerParams(
                collective_id=0, has_side_effects=True, vmem_limit_bytes=32 * 1024 * 1024
            ),
        )(*(
            pltpu.with_memory_space_constraint(x, pltpu.HBM) for x in (
                window_table,
                *(x.reshape(frames, plane, width) for x in (queries, keys, values, out_grad)),
                *(x.transpose(1, 2, 3, 0).reshape(cells, heads) for x in (log_norm, delta_rows)),
                text_keys, text_values,
            )
        ))

        dq, dk, dv, dtk, dtv = pl.pallas_call(
            hand_on,
            out_shape=[jax.ShapeDtypeStruct((rows, width), BF16)] * 3 + [jax.ShapeDtypeStruct((text, width), BF16)] * 2,
            in_specs=[vmem] * 5,
            out_specs=[anywhere] * 5,
            scratch_shapes=[sem((5,))],
            compiler_params=pltpu.CompilerParams(vmem_limit_bytes=4 * 1024 * 1024),
        )(*(pltpu.with_memory_space_constraint(x, pltpu.VMEM) for x in results))
        return *(x.reshape(queries.shape) for x in (dq, dk, dv)), dtk, dtv

    tile_spec = P("group", "ha", "wa", None)
    stat_spec = P(None, "group", "ha", "wa")
    text_spec = P("group", None)
    return jax.shard_map(
        local,
        mesh=mesh,
        in_specs=(tile_spec,) * 4 + (stat_spec,) * 2 + (text_spec,) * 2 + (P(),),
        out_specs=(tile_spec,) * 3 + (text_spec,) * 2,
        check_vma=False,
    )
```

```python
import functools
import math

import jax
import jax.numpy as jnp
from jax import lax
from jax.experimental import pallas as pl
from jax.experimental.pallas import tpu as pltpu
from jax.sharding import PartitionSpec as P

HDIM = 128
HALO = 2
GROUPS = 4
MESH = pl.DeviceIdType.MESH
F32 = jnp.float32
BF16 = jnp.bfloat16
I16 = jnp.int16
STEPS = 32766.0
LEAST = 1e-30
AHEAD = 2
LOG2E = math.log2(math.e)


def text_plan(n_ha, n_wa, blocks, width):
    plan = []

    def halve(axis, count):
        nonlocal blocks, width
        far = 1
        while far < count:
            if blocks > 1:
                blocks //= 2
                plan.append((axis, far, blocks, width, "rows"))
            elif width % 256 == 0:
                width //= 2
                plan.append((axis, far, blocks, width, "cols"))
            else:
                plan.append((axis, far, blocks, width, "none"))
            far *= 2

    halve("ha", n_ha)
    if width % (n_wa * 128) == 0:
        plan.append(("wa", n_wa, blocks, width // n_wa, "direct"))
    else:
        halve("wa", n_wa)
    return plan


def coded(stage_of):
    axis, far, _, _, _ = stage_of
    return axis != "ha" or far > 1


def contract(a, b, dims):
    return lax.dot_general(a, b, (dims, ((), ())), preferred_element_type=F32)


def encode(x):
    most = jnp.maximum(jnp.max(jnp.abs(x), axis=0, keepdims=True), LEAST)
    codes = jnp.round(x * (STEPS / most)).astype(jnp.int32).astype(I16)
    return codes, most * (1.0 / STEPS)


def decode(codes, steps):
    return codes.astype(jnp.int32).astype(F32) * steps


def kernel(n_ha, n_wa, plan, *refs):
    (table_h, q_h, k_h, v_h, g_h, norm_h, delta_h, tk_h, tv_h) = refs[:9]
    (dq_ref, dk_ref, dv_ref, dtk_ref, dtv_ref) = refs[9:14]
    (
        table, q_ref, k_ref, v_ref, g_ref, norm_ref, delta_ref, tk_ref, tv_ref,
        stage, hcol, hrow, hcor, part_col,
        out_col, out_row, out_cor, in_col, in_row, in_cor,
        st_col, st_row, st_cor, sr_col, sr_row, sr_cor,
        own, dq_acc, mask, norm, delta, tx, tb,
    ) = refs[14:47]
    buffers, rest = [], refs[47:]
    for stage_of in plan:
        count = 4 if coded(stage_of) else 1
        buffers.append(rest[:count])
        rest = rest[count:]
    (
        load_s, col_s, col_r, row_s, row_r, cor_s, cor_r,
        rc_s, rc_r, rr_s, rr_r, rq_s, rq_r,
        t_s, t_r, u_s, u_r,
    ) = rest

    frames, plane, width = q_ref.shape
    tile = math.isqrt(plane)
    cells = frames * plane
    text = tk_ref.shape[0]
    heads = width // HDIM
    part = width // GROUPS
    per = heads // GROUPS
    bands = tile // HALO
    band = frames * HALO * HALO
    strip = bands * band
    rim = frames * HALO * tile
    scale = 1.0 / math.sqrt(HDIM)
    ha, wa = lax.axis_index("ha"), lax.axis_index("wa")
    ha_of = [{"ha": lax.rem(ha + n_ha - 1, n_ha)}, {"ha": lax.rem(ha + 1, n_ha)}]
    wa_of = [{"wa": lax.rem(wa + n_wa - 1, n_wa)}, {"wa": lax.rem(wa + 1, n_wa)}]

    partners, bits = [], []
    for axis, far, _, _, how in plan:
        at = ha if axis == "ha" else wa
        if how == "direct":
            bits.append(None)
            partners.append([{axis: lax.rem(at + hop, far)} for hop in range(1, far)])
        else:
            bit = lax.rem(lax.div(at, far), 2)
            bits.append(bit)
            partners.append([{axis: at + far * (1 - 2 * bit)}])

    barrier = pltpu.get_barrier_semaphore()
    greeted = ha_of + wa_of + sum(partners, [])
    for other in greeted:
        pl.semaphore_signal(barrier, inc=1, device_id=other, device_id_type=MESH)

    loads = []
    for n, (src, dst) in enumerate((
        (k_h, k_ref), (v_h, v_ref), (q_h, q_ref), (g_h, g_ref), (tk_h, tk_ref), (tv_h, tv_ref),
        (norm_h, norm_ref), (delta_h, delta_ref), (table_h, table),
    )):
        c = pltpu.make_async_copy(src, dst, load_s.at[n])
        c.start()
        loads.append(c)

    def cols(g):
        return slice(g * part, (g + 1) * part)

    def lanes(h):
        return slice(h * HDIM, (h + 1) * HDIM)

    def remote(src, dst, s, r, device):
        c = pltpu.make_async_remote_copy(
            src_ref=src, dst_ref=dst, send_sem=s, recv_sem=r, device_id=device, device_id_type=MESH
        )
        c.start()
        return c

    def cell_of(j):
        side = lax.div(j, strip)
        order = lax.rem(lax.div(j, band), bands)
        at_band = jnp.where(order == 0, 0, jnp.where(order == 1, bands - 1, order - 1))
        frame = lax.rem(lax.div(j, HALO * HALO), frames)
        row = at_band * HALO + lax.rem(lax.div(j, HALO), HALO)
        col = lax.rem(j, HALO) + side * (tile - HALO)
        return frame * plane + row * tile + col

    border = 2 * strip
    lane = lax.broadcasted_iota(jnp.int32, (border, cells), 1)
    pick = (lane == cell_of(lax.broadcasted_iota(jnp.int32, (border, cells), 0))).astype(F32).astype(BF16)
    back_row = lax.broadcasted_iota(jnp.int32, (cells, 2 * border), 0)
    back_lane = lax.broadcasted_iota(jnp.int32, (cells, 2 * border), 1)
    put_back = (back_row == cell_of(lax.rem(back_lane, border))).astype(F32).astype(BF16)

    def whole(ref, where):
        return ref[:, :, where].reshape(cells, where.stop - where.start)

    col_copy, row_copy, cor_copy, rc_copy, rr_copy, rq_copy = {}, {}, {}, {}, {}, {}

    def send_rows(g):
        for v in range(2):
            lo = v * (tile - HALO) * tile
            for kv, ref in enumerate((k_ref, v_ref)):
                row_copy[g, v, kv] = remote(
                    ref.at[:, lo:lo + HALO * tile, cols(g)], hrow.at[g, kv, 1 - v],
                    row_s.at[g, v, kv], row_r.at[g, 1 - v, kv], ha_of[v],
                )

    def pick_cols(g):
        for kv, ref in enumerate((k_ref, v_ref)):
            found = contract(pick, whole(ref, cols(g)), ((1,), (0,))).astype(BF16)
            for d in range(2):
                stage[g, kv, d] = found[d * strip:(d + 1) * strip]

    def send_cols(g, half):
        lo, hi = ((0, 2 * band), (2 * band, strip))[half]
        for d in range(2):
            col_copy[g, d, half] = remote(
                stage.at[g, :, d, lo:hi], hcol.at[g, :, 1 - d, lo:hi],
                col_s.at[g, d, half], col_r.at[g, 1 - d, half], wa_of[d],
            )

    loads[0].wait()
    loads[1].wait()
    pick_cols(0)
    pl.semaphore_wait(barrier, len(greeted))
    send_cols(0, 0)
    send_rows(0)
    for g in range(1, GROUPS):
        pick_cols(g)
        send_cols(g, 0)
        send_rows(g)
    for g in range(GROUPS):
        send_cols(g, 1)

    for c in loads[2:]:
        c.wait()
    square = (cells, cells)
    same = (lax.broadcasted_iota(jnp.int32, square, 0) == lax.broadcasted_iota(jnp.int32, square, 1)).astype(F32)
    for src, dst, times in ((norm_ref, norm, LOG2E), (delta_ref, delta, 1.0)):
        dst[...] = times * lax.dot_general(
            src[...], same, (((0,), (0,)), ((), ())), precision=lax.Precision.HIGHEST, preferred_element_type=F32
        )

    def live(block):
        return table[ha, wa, block].astype(F32)

    at = 0
    for block, rows in ((1, rim), (7, rim), (0, band), (2, band), (6, band), (8, band), (3, strip), (5, strip)):
        mask[at:at + rows, :] = jnp.full((rows, cells), live(block), F32)
        at += rows
    own_live = live(4)

    def attend(todo, masking, sink):
        def scores(h, keys, values):
            qh, gh = whole(q_ref, lanes(h)), whole(g_ref, lanes(h))
            return h, keys, qh, gh, contract(keys, qh, ((1,), (1,))), contract(values, gh, ((1,), (1,)))

        def grads(h, keys, qh, gh, s, dp):
            p = masking(jnp.exp2(s * (scale * LOG2E) - norm[h:h + 1, :]))
            ds = (p * (dp - delta[h:h + 1, :])).astype(BF16)
            dv = contract(p.astype(BF16), gh, ((1,), (0,)))
            dk = contract(ds, qh, ((1,), (0,)))
            return h, keys, ds, dk, dv

        def close(h, keys, ds, dk, dv):
            sink(h, contract(ds, keys, ((0,), (0,))), dk, dv)

        first, second = [], []
        for n in range(len(todo) + AHEAD + 1):
            if n < len(todo):
                first.append(scores(*todo[n]))
            if AHEAD <= n < len(todo) + AHEAD:
                second.append(grads(*first.pop(0)))
            if n > AHEAD:
                close(*second.pop(0))

    def local():
        todo = []
        for h in range(heads):
            keys, values = (
                jnp.concatenate([whole(ref, lanes(h)), more[:, lanes(h)]], 0)
                for ref, more in ((k_ref, tk_ref), (v_ref, tv_ref))
            )
            todo.append((h, keys, values))

        def masking(p):
            return jnp.concatenate([p[:cells] * own_live, p[cells:]], 0)

        def sink(h, dq, dk, dv):
            here = lanes(h)
            dq_acc[:, here] = dq
            own[0, :, here] = dk[:cells]
            own[1, :, here] = dv[:cells]
            tx[: text // 8, :, here] = (dk[cells:] * scale).reshape(text // 8, 8, HDIM)
            tx[text // 8:, :, here] = dv[cells:].reshape(text // 8, 8, HDIM)

        attend(todo, masking, sink)

    def halo(groups, rows_of, weights, sink):
        todo = []
        for g in groups:
            for n in range(per):
                keys, values = (rows_of(g, kv, lanes(n)) for kv in range(2))
                todo.append((g * per + n, keys, values))

        def take(h, dq, dk, dv):
            dq_acc[:, lanes(h)] += dq
            sink(h // per, lanes(h % per), (dk, dv))

        attend(todo, lambda p: p * weights, take)

    def forward(g):
        for d in range(2):
            col_copy[g, d, 0].wait()
        for d in range(2):
            for v in range(2):
                to = ((1 - v) * 2 + d) * band
                cor_copy[g, d, v] = remote(
                    hcol.at[g, :, d, v * band:(v + 1) * band], hcor.at[g, :, to:to + band],
                    cor_s.at[g, d, v], cor_r.at[g, d, 1 - v], ha_of[v],
                )

    def columns(*groups):
        for g in groups:
            for d in range(2):
                col_copy[g, d, 1].wait()

        def sink(g, here, grads):
            for kv in range(2):
                for d in range(2):
                    lo = d * strip
                    codes, steps = encode(grads[kv][lo + 2 * band:lo + strip])
                    out_col[g, d, kv, 2 * band:, here] = codes
                    st_col[g, d, 1, kv:kv + 1, here] = steps
                    part_col[g, d, kv, :, here] = grads[kv][lo:lo + 2 * band]

        halo(
            groups, lambda g, kv, here: hcol[g, kv, :, :, here].reshape(border, HDIM), mask[2 * rim + 4 * band:], sink
        )
        for g in groups:
            send_back(g, 1)

    def send_back(g, half):
        lo, hi = ((0, 2 * band), (2 * band, strip))[half]
        for d in range(2):
            rc_copy[g, d, half] = (
                remote(
                    out_col.at[g, d, :, lo:hi], in_col.at[g, 1 - d, :, lo:hi],
                    rc_s.at[g, d, half, 0], rc_r.at[g, 1 - d, half, 0], wa_of[d],
                ),
                remote(
                    st_col.at[g, d, half], sr_col.at[g, 1 - d, half],
                    rc_s.at[g, d, half, 1], rc_r.at[g, 1 - d, half, 1], wa_of[d],
                ),
            )

    def fold_ends(g):
        for v in range(2):
            for c in rq_copy[g, v]:
                c.wait()
        for kv in range(2):
            came = [decode(in_cor[g, v, kv], sr_cor[g, v, kv:kv + 1]) for v in range(2)]
            for d in range(2):
                ends = jnp.concatenate([came[v][d * band:(d + 1) * band] for v in range(2)], 0)
                codes, steps = encode(part_col[g, d, kv] + ends)
                out_col[g, d, kv, :2 * band, :] = codes
                st_col[g, d, 0, kv:kv + 1, :] = steps
        send_back(g, 0)

    def strips(*groups):
        for g in groups:
            for v in range(2):
                for kv in range(2):
                    row_copy[g, v, kv].wait()

        def sink(g, here, grads):
            for kv in range(2):
                for v in range(2):
                    codes, steps = encode(grads[kv][v * rim:(v + 1) * rim])
                    out_row[g, v, kv, :, here] = codes
                    st_row[g, v, kv:kv + 1, here] = steps

        halo(
            groups, lambda g, kv, here: hrow[g, kv, :, :, :, here].reshape(2 * rim, HDIM), mask[:2 * rim], sink
        )

    def send_strips(g):
        for v in range(2):
            rr_copy[g, v] = (
                remote(out_row.at[g, v], in_row.at[g, 1 - v], rr_s.at[g, v, 0], rr_r.at[g, 1 - v, 0], ha_of[v]),
                remote(st_row.at[g, v], sr_row.at[g, 1 - v], rr_s.at[g, v, 1], rr_r.at[g, 1 - v, 1], ha_of[v]),
            )

    def corners(*groups):
        for g in groups:
            for v in range(2):
                for d in range(2):
                    cor_copy[g, d, v].wait()

        def sink(g, here, grads):
            for kv in range(2):
                for v in range(2):
                    codes, steps = encode(grads[kv][2 * v * band:2 * (v + 1) * band])
                    out_cor[g, v, kv, :, here] = codes
                    st_cor[g, v, kv:kv + 1, here] = steps

        halo(groups, lambda g, kv, here: hcor[g, kv, :, here], mask[2 * rim:2 * rim + 4 * band], sink)
        for g in groups:
            for v in range(2):
                rq_copy[g, v] = (
                    remote(out_cor.at[g, v], in_cor.at[g, 1 - v], rq_s.at[g, v, 0], rq_r.at[g, 1 - v, 0], ha_of[v]),
                    remote(st_cor.at[g, v], sr_cor.at[g, 1 - v], rq_s.at[g, v, 1], rq_r.at[g, 1 - v, 1], ha_of[v]),
                )

    def fold_rows(g):
        for v in range(2):
            for c in rr_copy[g, v]:
                c.wait()
        for v in range(2):
            for kv in range(2):
                came = decode(in_row[g, v, kv], sr_row[g, v, kv:kv + 1])
                for f in range(frames):
                    lo = f * plane + v * (tile - HALO) * tile
                    own[kv, lo:lo + HALO * tile, cols(g)] += came[f * HALO * tile:(f + 1) * HALO * tile]

    def finish_queries(g):
        dq_ref[:, cols(g)] = (dq_acc[:, cols(g)] * scale).astype(BF16)

    def fold_cols(g):
        for d in range(2):
            for c in rc_copy[g, d, 0] + rc_copy[g, d, 1]:
                c.wait()
        for kv, out in enumerate((dk_ref, dv_ref)):
            came = jnp.concatenate([
                decode(in_col[g, d, kv, lo:hi], sr_col[g, d, half, kv:kv + 1])
                for d in range(2) for half, (lo, hi) in enumerate(((0, 2 * band), (2 * band, strip)))
            ], 0)
            first = came.astype(BF16)
            second = (came - first.astype(F32)).astype(BF16)
            total = own[kv, :, cols(g)] + contract(put_back, jnp.concatenate([first, second], 0), ((1,), (0,)))
            if kv == 0:
                total = total * scale
            out[:, cols(g)] = total.astype(BF16)

    region = {"row": 0, "rows": 2 * text // 8, "col": 0, "cols": width}
    sums, regions = [], []

    def area(ref, row, rows, col, wide):
        where = pl.ds(pl.multiple_of(col, 128), wide) if not isinstance(col, int) else pl.ds(col, wide)
        return ref.at[pl.ds(row, rows), :, where]

    def mine(ref):
        return area(ref, region["row"], region["rows"], region["col"], region["cols"])

    def text_send(i):
        _, far, rows, wide, how = plan[i]
        regions.append(dict(region))
        row, col, bit = region["row"], region["col"], bits[i]
        if how == "direct":
            where = [(row, col + lax.rem(wa + hop, far) * wide) for hop in range(1, far)]
            region.update(col=col + wa * wide, cols=wide)
        elif how == "rows":
            where = [(row + (1 - bit) * rows, col)]
            region.update(row=row + bit * rows, rows=rows)
        elif how == "cols":
            where = [(row, col + (1 - bit) * wide)]
            region.update(col=col + bit * wide, cols=wide)
        else:
            where = [(row, col)]
        out = []
        for n, at in enumerate(where):
            source = area(tx, at[0], rows, at[1], wide)
            if coded(plan[i]):
                codes, steps, codes_in, steps_in = buffers[i]
                codes[n], steps[n] = encode(source[...].reshape(rows * 8, wide))
                out.append(remote(codes.at[n], codes_in.at[n], t_s.at[i, n, 0], t_r.at[i, n, 0], partners[i][n]))
                out.append(remote(steps.at[n], steps_in.at[n], t_s.at[i, n, 1], t_r.at[i, n, 1], partners[i][n]))
            else:
                out.append(remote(source, buffers[i][0].at[n], t_s.at[i, n, 0], t_r.at[i, n, 0], partners[i][n]))
        sums.append(out)

    def text_add(i):
        _, _, rows, wide, _ = plan[i]
        for c in sums[i]:
            c.wait()
        kept = mine(tx)
        total = kept[...]
        for n in range(len(partners[i])):
            if coded(plan[i]):
                _, _, codes_in, steps_in = buffers[i]
                total = total + decode(codes_in[n], steps_in[n]).reshape(rows, 8, wide)
            else:
                total = total + buffers[i][0][n]
        kept[...] = total

    gathers = []

    def text_spread(i):
        if i == len(plan) - 1:
            mine(tb)[...] = mine(tx)[...].astype(BF16)
        out = []
        if plan[i][4] != "none":
            for n, partner in enumerate(partners[i]):
                out.append(remote(mine(tb), mine(tb), u_s.at[i, n], u_r.at[i, n], partner))
        gathers.append(out)

    def text_join(i):
        for c in gathers.pop():
            c.wait()
        region.update(regions[i])

    steps = []
    for i in range(len(plan)):
        steps += [functools.partial(text_send, i), functools.partial(text_add, i)]
    for i in reversed(range(len(plan))):
        steps += [functools.partial(text_spread, i), functools.partial(text_join, i)]
    waiting = [steps[:1]] + [steps[n:n + 2] for n in range(1, len(steps) - 1, 2)] + [steps[-1:]]

    def text_step():
        if waiting:
            for step in waiting.pop(0):
                step()

    local()
    text_step()
    strips(0)
    forward(0)
    text_step()
    strips(1)
    forward(1)
    strips(2)
    forward(2)
    strips(3)
    forward(3)
    text_step()
    corners(0)
    send_strips(0)
    columns(0)
    corners(1)
    send_strips(1)
    columns(1)
    text_step()
    corners(2)
    send_strips(2)
    fold_ends(0)
    columns(2)
    corners(3)
    send_strips(3)
    fold_ends(1)
    columns(3)
    fold_ends(2)
    text_step()
    fold_ends(3)
    for g in range(GROUPS):
        finish_queries(g)
    for g in range(GROUPS):
        fold_rows(g)
    text_step()
    fold_cols(0)
    fold_cols(1)
    while waiting:
        text_step()
    dtk_ref[...] = tb[: text // 8].astype(F32).reshape(text, width).astype(BF16)
    dtv_ref[...] = tb[text // 8:].astype(F32).reshape(text, width).astype(BF16)
    for g in range(2, GROUPS):
        fold_cols(g)


def hand_on(*refs):
    count = (len(refs) - 1) // 2
    copies = []
    for n in range(count):
        c = pltpu.make_async_copy(refs[n], refs[count + n], refs[-1].at[n])
        c.start()
        copies.append(c)
    for c in copies:
        c.wait()


def solution(mesh):
    n_ha, n_wa = mesh.shape["ha"], mesh.shape["wa"]

    def local(queries, keys, values, out_grad, log_norm, delta_rows, text_keys, text_values, window_table):
        frames, tile, _, width = queries.shape
        heads = width // HDIM
        text = text_keys.shape[0]
        plane = tile * tile
        cells = frames * plane
        part = width // GROUPS
        bands = tile // HALO
        band = frames * HALO * HALO
        strip = bands * band
        rim = frames * HALO * tile
        plan = text_plan(n_ha, n_wa, 2 * text // 8, width)
        most = max([far - 1 if how == "direct" else 1 for _, far, _, _, how in plan] + [1])
        received = []
        for stage_of in plan:
            _, far, rows, wide, how = stage_of
            n = far - 1 if how == "direct" else 1
            if coded(stage_of):
                received += [pltpu.VMEM((n, rows * 8, wide), I16), pltpu.VMEM((n, 1, wide), F32)] * 2
            else:
                received.append(pltpu.VMEM((n, rows, 8, wide), F32))
        sem = pltpu.SemaphoreType.DMA
        anywhere = pl.BlockSpec(memory_space=pltpu.HBM)
        vmem = pl.BlockSpec(memory_space=pltpu.VMEM)
        rows = frames * plane
        results = pl.pallas_call(
            functools.partial(kernel, n_ha, n_wa, plan),
            out_shape=[pltpu.VMEM((rows, width), BF16)] * 3 + [pltpu.VMEM((text, width), BF16)] * 2,
            in_specs=[anywhere] * 9,
            out_specs=[vmem] * 5,
            scratch_shapes=[
                pltpu.SMEM(window_table.shape, jnp.int32),
                *[pltpu.VMEM((frames, plane, width), BF16)] * 4,
                *[pltpu.VMEM((cells, heads), F32)] * 2,
                *[pltpu.VMEM((text, width), BF16)] * 2,
                pltpu.VMEM((GROUPS, 2, 2, strip, part), BF16),
                pltpu.VMEM((GROUPS, 2, 2, strip, part), BF16),
                pltpu.VMEM((GROUPS, 2, 2, frames, HALO * tile, part), BF16),
                pltpu.VMEM((GROUPS, 2, 4 * band, part), BF16),
                pltpu.VMEM((GROUPS, 2, 2, 2 * band, part), F32),
                pltpu.VMEM((GROUPS, 2, 2, strip, part), I16),
                pltpu.VMEM((GROUPS, 2, 2, rim, part), I16),
                pltpu.VMEM((GROUPS, 2, 2, 2 * band, part), I16),
                pltpu.VMEM((GROUPS, 2, 2, strip, part), I16),
                pltpu.VMEM((GROUPS, 2, 2, rim, part), I16),
                pltpu.VMEM((GROUPS, 2, 2, 2 * band, part), I16),
                pltpu.VMEM((GROUPS, 2, 2, 2, part), F32),
                pltpu.VMEM((GROUPS, 2, 2, part), F32),
                pltpu.VMEM((GROUPS, 2, 2, part), F32),
                pltpu.VMEM((GROUPS, 2, 2, 2, part), F32),
                pltpu.VMEM((GROUPS, 2, 2, part), F32),
                pltpu.VMEM((GROUPS, 2, 2, part), F32),
                pltpu.VMEM((2, cells, width), F32),
                pltpu.VMEM((cells, width), F32),
                pltpu.VMEM((2 * rim + 4 * band + 2 * strip, cells), F32),
                pltpu.VMEM((heads, cells), F32),
                pltpu.VMEM((heads, cells), F32),
                pltpu.VMEM((2 * text // 8, 8, width), F32),
                pltpu.VMEM((2 * text // 8, 8, width), BF16),
                *received,
                sem((9,)),
                sem((GROUPS, 2, 2)), sem((GROUPS, 2, 2)),
                sem((GROUPS, 2, 2)), sem((GROUPS, 2, 2)),
                sem((GROUPS, 2, 2)), sem((GROUPS, 2, 2)),
                sem((GROUPS, 2, 2, 2)), sem((GROUPS, 2, 2, 2)),
                sem((GROUPS, 2, 2)), sem((GROUPS, 2, 2)),
                sem((GROUPS, 2, 2)), sem((GROUPS, 2, 2)),
                sem((len(plan), most, 2)), sem((len(plan), most, 2)),
                sem((len(plan), most)), sem((len(plan), most)),
            ],
            compiler_params=pltpu.CompilerParams(
                collective_id=0, has_side_effects=True, vmem_limit_bytes=32 * 1024 * 1024
            ),
        )(*(
            pltpu.with_memory_space_constraint(x, pltpu.HBM) for x in (
                window_table,
                *(x.reshape(frames, plane, width) for x in (queries, keys, values, out_grad)),
                *(x.transpose(1, 2, 3, 0).reshape(cells, heads) for x in (log_norm, delta_rows)),
                text_keys, text_values,
            )
        ))

        dq, dk, dv, dtk, dtv = pl.pallas_call(
            hand_on,
            out_shape=[jax.ShapeDtypeStruct((rows, width), BF16)] * 3 + [jax.ShapeDtypeStruct((text, width), BF16)] * 2,
            in_specs=[vmem] * 5,
            out_specs=[anywhere] * 5,
            scratch_shapes=[sem((5,))],
            compiler_params=pltpu.CompilerParams(vmem_limit_bytes=4 * 1024 * 1024),
        )(*(pltpu.with_memory_space_constraint(x, pltpu.VMEM) for x in results))
        return *(x.reshape(queries.shape) for x in (dq, dk, dv)), dtk, dtv

    tile_spec = P("group", "ha", "wa", None)
    stat_spec = P(None, "group", "ha", "wa")
    text_spec = P("group", None)
    return jax.shard_map(
        local,
        mesh=mesh,
        in_specs=(tile_spec,) * 4 + (stat_spec,) * 2 + (text_spec,) * 2 + (P(),),
        out_specs=(tile_spec,) * 3 + (text_spec,) * 2,
        check_vma=False,
    )
```

```python
import functools
import math

import jax
import jax.numpy as jnp
from jax import lax
from jax.experimental import pallas as pl
from jax.experimental.pallas import tpu as pltpu
from jax.sharding import PartitionSpec as P

HDIM = 128
HALO = 2
GROUPS = 4
MESH = pl.DeviceIdType.MESH
F32 = jnp.float32
BF16 = jnp.bfloat16
I16 = jnp.int16
STEPS = 32766.0
LEAST = 1e-30
AHEAD = 2
LOG2E = math.log2(math.e)


def text_plan(n_ha, n_wa, blocks, width):
    plan = []

    def halve(axis, count):
        nonlocal blocks, width
        far = 1
        while far < count:
            if blocks > 1:
                blocks //= 2
                plan.append((axis, far, blocks, width, "rows"))
            elif width % 256 == 0:
                width //= 2
                plan.append((axis, far, blocks, width, "cols"))
            else:
                plan.append((axis, far, blocks, width, "none"))
            far *= 2

    halve("ha", n_ha)
    if width % (n_wa * 128) == 0:
        plan.append(("wa", n_wa, blocks, width // n_wa, "direct"))
    else:
        halve("wa", n_wa)
    return plan


def coded(stage_of):
    axis, far, _, _, _ = stage_of
    return axis != "ha" or far > 1


def contract(a, b, dims):
    return lax.dot_general(a, b, (dims, ((), ())), preferred_element_type=F32)


def slices(x):
    return [x[:, n:n + HDIM] for n in range(0, x.shape[1], HDIM)]


def encode(x):
    most = jnp.max(jnp.abs(x), axis=0, keepdims=True)
    most = jnp.maximum(functools.reduce(jnp.maximum, slices(most)), LEAST)
    by = STEPS / most
    codes = jnp.concatenate([jnp.round(piece * by).astype(jnp.int32).astype(I16) for piece in slices(x)], 1)
    return codes, most * (1.0 / STEPS)


def by_head(codes, steps):
    return codes.astype(jnp.int32).astype(F32) * steps


def decode(codes, steps):
    return jnp.concatenate([piece.astype(jnp.int32).astype(F32) * steps for piece in slices(codes)], 1)


def kernel(n_ha, n_wa, plan, *refs):
    (table_h, q_h, k_h, v_h, g_h, norm_h, delta_h, tk_h, tv_h) = refs[:9]
    (dq_ref, dk_ref, dv_ref, dtk_ref, dtv_ref) = refs[9:14]
    (
        table, q_ref, k_ref, v_ref, g_ref, norm_ref, delta_ref, tk_ref, tv_ref,
        stage, hcol, hrow, hcor, part_col,
        out_col, out_row, out_cor, in_col, in_row, in_cor,
        st_col, st_row, st_cor, sr_col, sr_row, sr_cor,
        own, dq_acc, mask, norm, delta, tx, tb,
    ) = refs[14:47]
    buffers, rest = [], refs[47:]
    for stage_of in plan:
        count = 4 if coded(stage_of) else 1
        buffers.append(rest[:count])
        rest = rest[count:]
    (
        load_s, col_s, col_r, row_s, row_r, cor_s, cor_r,
        rc_s, rc_r, rr_s, rr_r, rq_s, rq_r,
        t_s, t_r, u_s, u_r,
    ) = rest

    frames, plane, width = q_ref.shape
    tile = math.isqrt(plane)
    cells = frames * plane
    text = tk_ref.shape[0]
    heads = width // HDIM
    part = width // GROUPS
    per = heads // GROUPS
    bands = tile // HALO
    band = frames * HALO * HALO
    strip = bands * band
    rim = frames * HALO * tile
    scale = 1.0 / math.sqrt(HDIM)
    ha, wa = lax.axis_index("ha"), lax.axis_index("wa")
    ha_of = [{"ha": lax.rem(ha + n_ha - 1, n_ha)}, {"ha": lax.rem(ha + 1, n_ha)}]
    wa_of = [{"wa": lax.rem(wa + n_wa - 1, n_wa)}, {"wa": lax.rem(wa + 1, n_wa)}]

    partners, bits = [], []
    for axis, far, _, _, how in plan:
        at = ha if axis == "ha" else wa
        if how == "direct":
            bits.append(None)
            partners.append([{axis: lax.rem(at + hop, far)} for hop in range(1, far)])
        else:
            bit = lax.rem(lax.div(at, far), 2)
            bits.append(bit)
            partners.append([{axis: at + far * (1 - 2 * bit)}])

    barrier = pltpu.get_barrier_semaphore()
    greeted = ha_of + wa_of + sum(partners, [])
    for other in greeted:
        pl.semaphore_signal(barrier, inc=1, device_id=other, device_id_type=MESH)
    last = jnp.where(wa < n_wa - 1, 0, 1)

    loads = []
    for n, (src, dst) in enumerate((
        (k_h, k_ref), (v_h, v_ref), (q_h, q_ref), (g_h, g_ref), (tk_h, tk_ref), (tv_h, tv_ref),
        (norm_h, norm_ref), (delta_h, delta_ref), (table_h, table),
    )):
        c = pltpu.make_async_copy(src, dst, load_s.at[n])
        c.start()
        loads.append(c)

    def cols(g):
        return slice(g * part, (g + 1) * part)

    def lanes(h):
        return slice(h * HDIM, (h + 1) * HDIM)

    def later(src, dst, s, r, device):
        return pltpu.make_async_remote_copy(
            src_ref=src, dst_ref=dst, send_sem=s, recv_sem=r, device_id=device, device_id_type=MESH
        )

    def remote(*what):
        c = later(*what)
        c.start()
        return c

    def cell_of(j):
        side = lax.div(j, strip)
        order = lax.rem(lax.div(j, band), bands)
        at_band = jnp.where(order == 0, 0, jnp.where(order == 1, bands - 1, order - 1))
        frame = lax.rem(lax.div(j, HALO * HALO), frames)
        row = at_band * HALO + lax.rem(lax.div(j, HALO), HALO)
        col = lax.rem(j, HALO) + side * (tile - HALO)
        return frame * plane + row * tile + col

    border = 2 * strip
    lane = lax.broadcasted_iota(jnp.int32, (border, cells), 1)
    pick = (lane == cell_of(lax.broadcasted_iota(jnp.int32, (border, cells), 0))).astype(F32).astype(BF16)
    back_row = lax.broadcasted_iota(jnp.int32, (cells, 2 * border), 0)
    back_lane = lax.broadcasted_iota(jnp.int32, (cells, 2 * border), 1)
    put_back = (back_row == cell_of(lax.rem(back_lane, border))).astype(F32).astype(BF16)

    def whole(ref, where):
        return ref[:, :, where].reshape(cells, where.stop - where.start)

    col_copy, row_copy, cor_copy, rc_copy, rr_copy, rq_copy = {}, {}, {}, {}, {}, {}

    def send_rows(g):
        for v in range(2):
            lo = v * (tile - HALO) * tile
            for kv, ref in enumerate((k_ref, v_ref)):
                row_copy[g, v, kv] = remote(
                    ref.at[:, lo:lo + HALO * tile, cols(g)], hrow.at[g, kv, 1 - v],
                    row_s.at[g, v, kv], row_r.at[g, 1 - v, kv], ha_of[v],
                )

    def pick_cols(g):
        for kv, ref in enumerate((k_ref, v_ref)):
            found = contract(pick, whole(ref, cols(g)), ((1,), (0,))).astype(BF16)
            for d in range(2):
                stage[g, kv, d] = found[d * strip:(d + 1) * strip]

    def send_cols(g, half):
        lo, hi = ((0, 2 * band), (2 * band, strip))[half]
        for n in range(2):
            d = lax.rem(last + n, 2)
            to = {"wa": lax.rem(wa + n_wa + 2 * d - 1, n_wa)}
            col_copy[g, n, half] = remote(
                stage.at[g, :, d, lo:hi], hcol.at[g, :, 1 - d, lo:hi],
                col_s.at[g, d, half], col_r.at[g, 1 - d, half], to,
            )

    loads[0].wait()
    loads[1].wait()
    pick_cols(0)
    pl.semaphore_wait(barrier, len(greeted))
    send_cols(0, 0)
    send_rows(0)
    for g in range(1, GROUPS):
        pick_cols(g)
        send_cols(g, 0)
        send_rows(g)
    for g in range(GROUPS):
        send_cols(g, 1)

    for c in loads[2:]:
        c.wait()
    square = (cells, cells)
    same = (lax.broadcasted_iota(jnp.int32, square, 0) == lax.broadcasted_iota(jnp.int32, square, 1)).astype(F32)
    for src, dst, times in ((norm_ref, norm, LOG2E), (delta_ref, delta, 1.0)):
        dst[...] = times * lax.dot_general(
            src[...], same, (((0,), (0,)), ((), ())), precision=lax.Precision.HIGHEST, preferred_element_type=F32
        )

    def live(block):
        return table[ha, wa, block].astype(F32)

    at = 0
    for block, rows in ((1, rim), (7, rim), (0, band), (2, band), (6, band), (8, band), (3, strip), (5, strip)):
        mask[at:at + rows, :] = jnp.full((rows, cells), live(block), F32)
        at += rows
    own_live = live(4)

    def attend(todo, masking, sink):
        def scores(h, keys, values):
            qh, gh = whole(q_ref, lanes(h)), whole(g_ref, lanes(h))
            return h, keys, qh, gh, contract(keys, qh, ((1,), (1,))), contract(values, gh, ((1,), (1,)))

        def grads(h, keys, qh, gh, s, dp):
            p = masking(jnp.exp2(s * (scale * LOG2E) - norm[h:h + 1, :]))
            ds = (p * (dp - delta[h:h + 1, :])).astype(BF16)
            dv = contract(p.astype(BF16), gh, ((1,), (0,)))
            dk = contract(ds, qh, ((1,), (0,)))
            return h, keys, ds, dk, dv

        def close(h, keys, ds, dk, dv):
            sink(h, contract(ds, keys, ((0,), (0,))), dk, dv)

        first, second = [], []
        for n in range(len(todo) + AHEAD + 1):
            if n < len(todo):
                first.append(scores(*todo[n]))
            if AHEAD <= n < len(todo) + AHEAD:
                second.append(grads(*first.pop(0)))
            if n > AHEAD:
                close(*second.pop(0))

    def local():
        todo = []
        for h in range(heads):
            keys, values = (
                jnp.concatenate([whole(ref, lanes(h)), more[:, lanes(h)]], 0)
                for ref, more in ((k_ref, tk_ref), (v_ref, tv_ref))
            )
            todo.append((h, keys, values))

        def masking(p):
            return jnp.concatenate([p[:cells] * own_live, p[cells:]], 0)

        def sink(h, dq, dk, dv):
            here = lanes(h)
            dq_acc[:, here] = dq
            own[0, :, here] = dk[:cells]
            own[1, :, here] = dv[:cells]
            tx[: text // 8, :, here] = (dk[cells:] * scale).reshape(text // 8, 8, HDIM)
            tx[text // 8:, :, here] = dv[cells:].reshape(text // 8, 8, HDIM)

        attend(todo, masking, sink)

    def halo(groups, rows_of, weights, sink):
        todo = []
        for g in groups:
            for n in range(per):
                keys, values = (rows_of(g, kv, lanes(n)) for kv in range(2))
                todo.append((g * per + n, keys, values))

        def take(h, dq, dk, dv):
            dq_acc[:, lanes(h)] += dq
            sink(h // per, lanes(h % per), (dk, dv))

        attend(todo, lambda p: p * weights, take)

    def forward(g):
        for d in range(2):
            col_copy[g, d, 0].wait()
        for d in range(2):
            for v in range(2):
                to = ((1 - v) * 2 + d) * band
                cor_copy[g, d, v] = remote(
                    hcol.at[g, :, d, v * band:(v + 1) * band], hcor.at[g, :, to:to + band],
                    cor_s.at[g, d, v], cor_r.at[g, d, 1 - v], ha_of[v],
                )

    def columns(*groups):
        for g in groups:
            for d in range(2):
                col_copy[g, d, 1].wait()

        def sink(g, here, grads):
            for kv in range(2):
                for d in range(2):
                    part_col[g, d, kv, :, here] = grads[kv][d * strip:(d + 1) * strip]

        halo(
            groups, lambda g, kv, here: hcol[g, kv, :, :, here].reshape(border, HDIM), mask[2 * rim + 4 * band:], sink
        )
        for g in groups:
            for kv in range(2):
                for d in range(2):
                    codes, steps = encode(part_col[g, d, kv, 2 * band:])
                    out_col[g, d, kv, 2 * band:, :] = codes
                    st_col[g, d, 1, kv:kv + 1, :] = steps
            send_back(g, 1)

    def send_back(g, half):
        lo, hi = ((0, 2 * band), (2 * band, strip))[half]
        for n in range(2):
            d = lax.rem(last + n, 2)
            to = {"wa": lax.rem(wa + n_wa + 2 * d - 1, n_wa)}
            rc_copy[g, n, half] = (
                remote(
                    out_col.at[g, d, :, lo:hi], in_col.at[g, 1 - d, :, lo:hi],
                    rc_s.at[g, d, half, 0], rc_r.at[g, 1 - d, half, 0], to,
                ),
                remote(
                    st_col.at[g, d, half], sr_col.at[g, 1 - d, half],
                    rc_s.at[g, d, half, 1], rc_r.at[g, 1 - d, half, 1], to,
                ),
            )

    def fold_ends(g):
        for v in range(2):
            for c in rq_copy[g, v]:
                c.wait()
        for kv in range(2):
            came = [by_head(in_cor[g, v, kv], sr_cor[g, v, kv:kv + 1]) for v in range(2)]
            for d in range(2):
                ends = jnp.concatenate([came[v][d * band:(d + 1) * band] for v in range(2)], 0)
                codes, steps = encode(part_col[g, d, kv, :2 * band] + ends)
                out_col[g, d, kv, :2 * band, :] = codes
                st_col[g, d, 0, kv:kv + 1, :] = steps
        send_back(g, 0)

    def strips(*groups):
        for g in groups:
            for v in range(2):
                for kv in range(2):
                    row_copy[g, v, kv].wait()

        def sink(g, here, grads):
            for kv in range(2):
                for v in range(2):
                    codes, steps = encode(grads[kv][v * rim:(v + 1) * rim])
                    out_row[g, v, kv, :, here] = codes
                    st_row[g, v, kv:kv + 1, here] = steps

        halo(
            groups, lambda g, kv, here: hrow[g, kv, :, :, :, here].reshape(2 * rim, HDIM), mask[:2 * rim], sink
        )

    def send_strips(g):
        for v in range(2):
            rr_copy[g, v] = (
                remote(out_row.at[g, v], in_row.at[g, 1 - v], rr_s.at[g, v, 0], rr_r.at[g, 1 - v, 0], ha_of[v]),
                remote(st_row.at[g, v], sr_row.at[g, 1 - v], rr_s.at[g, v, 1], rr_r.at[g, 1 - v, 1], ha_of[v]),
            )

    def corners(*groups):
        for g in groups:
            for v in range(2):
                for d in range(2):
                    cor_copy[g, d, v].wait()

        def sink(g, here, grads):
            for kv in range(2):
                for v in range(2):
                    codes, steps = encode(grads[kv][2 * v * band:2 * (v + 1) * band])
                    out_cor[g, v, kv, :, here] = codes
                    st_cor[g, v, kv:kv + 1, here] = steps

        halo(groups, lambda g, kv, here: hcor[g, kv, :, here], mask[2 * rim:2 * rim + 4 * band], sink)
        for g in groups:
            for v in range(2):
                rq_copy[g, v] = (
                    remote(out_cor.at[g, v], in_cor.at[g, 1 - v], rq_s.at[g, v, 0], rq_r.at[g, 1 - v, 0], ha_of[v]),
                    remote(st_cor.at[g, v], sr_cor.at[g, 1 - v], rq_s.at[g, v, 1], rq_r.at[g, 1 - v, 1], ha_of[v]),
                )

    def fold_rows(g):
        for v in range(2):
            for c in rr_copy[g, v]:
                c.wait()
        for v in range(2):
            for kv in range(2):
                came = by_head(in_row[g, v, kv], sr_row[g, v, kv:kv + 1])
                for f in range(frames):
                    lo = f * plane + v * (tile - HALO) * tile
                    own[kv, lo:lo + HALO * tile, cols(g)] += came[f * HALO * tile:(f + 1) * HALO * tile]

    def finish_queries(g):
        dq_ref[:, cols(g)] = (dq_acc[:, cols(g)] * scale).astype(BF16)

    def fold_cols(g):
        for d in range(2):
            for c in rc_copy[g, d, 0] + rc_copy[g, d, 1]:
                c.wait()
        for kv, out in enumerate((dk_ref, dv_ref)):
            came = jnp.concatenate([
                decode(in_col[g, d, kv, lo:hi], sr_col[g, d, half, kv:kv + 1])
                for d in range(2) for half, (lo, hi) in enumerate(((0, 2 * band), (2 * band, strip)))
            ], 0)
            first = came.astype(BF16)
            second = (came - first.astype(F32)).astype(BF16)
            total = own[kv, :, cols(g)] + contract(put_back, jnp.concatenate([first, second], 0), ((1,), (0,)))
            if kv == 0:
                total = total * scale
            out[:, cols(g)] = total.astype(BF16)

    region = {"row": 0, "rows": 2 * text // 8, "col": 0, "cols": width}
    sums, regions = [], []

    def area(ref, row, rows, col, wide):
        where = pl.ds(pl.multiple_of(col, 128), wide) if not isinstance(col, int) else pl.ds(col, wide)
        return ref.at[pl.ds(row, rows), :, where]

    def mine(ref):
        return area(ref, region["row"], region["rows"], region["col"], region["cols"])

    def text_send(i):
        _, far, rows, wide, how = plan[i]
        regions.append(dict(region))
        row, col, bit = region["row"], region["col"], bits[i]
        if how == "direct":
            where = [(row, col + lax.rem(wa + hop, far) * wide) for hop in range(1, far)]
            region.update(col=col + wa * wide, cols=wide)
        elif how == "rows":
            where = [(row + (1 - bit) * rows, col)]
            region.update(row=row + bit * rows, rows=rows)
        elif how == "cols":
            where = [(row, col + (1 - bit) * wide)]
            region.update(col=col + bit * wide, cols=wide)
        else:
            where = [(row, col)]
        out = []
        for n, at in enumerate(where):
            source = area(tx, at[0], rows, at[1], wide)
            if coded(plan[i]):
                codes, steps, codes_in, steps_in = buffers[i]
                codes[n], steps[n] = encode(source[...].reshape(rows * 8, wide))
                out.append(remote(codes.at[n], codes_in.at[n], t_s.at[i, n, 0], t_r.at[i, n, 0], partners[i][n]))
                out.append(remote(steps.at[n], steps_in.at[n], t_s.at[i, n, 1], t_r.at[i, n, 1], partners[i][n]))
            else:
                out.append(remote(source, buffers[i][0].at[n], t_s.at[i, n, 0], t_r.at[i, n, 0], partners[i][n]))
        sums.append(out)

    def text_add(i):
        _, _, rows, wide, _ = plan[i]
        for c in sums[i]:
            c.wait()
        kept = mine(tx)
        total = kept[...]
        for n in range(len(partners[i])):
            if coded(plan[i]):
                _, _, codes_in, steps_in = buffers[i]
                total = total + decode(codes_in[n], steps_in[n]).reshape(rows, 8, wide)
            else:
                total = total + buffers[i][0][n]
        kept[...] = total

    gathers = []

    def text_spread(i):
        if i == len(plan) - 1:
            mine(tb)[...] = mine(tx)[...].astype(BF16)
        out = []
        if plan[i][4] != "none":
            for n, partner in enumerate(partners[i]):
                out.append(remote(mine(tb), mine(tb), u_s.at[i, n], u_r.at[i, n], partner))
        gathers.append(out)

    def text_join(i):
        for c in gathers.pop():
            c.wait()
        region.update(regions[i])

    steps = []
    for i in range(len(plan)):
        steps += [functools.partial(text_send, i), functools.partial(text_add, i)]
    for i in reversed(range(len(plan))):
        steps += [functools.partial(text_spread, i), functools.partial(text_join, i)]
    waiting = [steps[:1]] + [steps[n:n + 2] for n in range(1, len(steps) - 1, 2)] + [steps[-1:]]

    def text_step():
        if waiting:
            for step in waiting.pop(0):
                step()

    local()
    text_step()
    strips(0)
    forward(0)
    text_step()
    strips(1)
    forward(1)
    strips(2)
    forward(2)
    strips(3)
    forward(3)
    text_step()
    corners(0)
    send_strips(0)
    columns(0)
    corners(1)
    send_strips(1)
    columns(1)
    text_step()
    corners(2)
    send_strips(2)
    fold_ends(0)
    columns(2)
    corners(3)
    send_strips(3)
    fold_ends(1)
    columns(3)
    fold_ends(2)
    text_step()
    fold_ends(3)
    for g in range(GROUPS):
        finish_queries(g)
    fold_rows(0)
    fold_rows(1)
    fold_rows(2)
    fold_rows(3)
    text_step()
    fold_cols(0)
    fold_cols(1)
    while waiting:
        text_step()
    dtk_ref[...] = tb[: text // 8].astype(F32).reshape(text, width).astype(BF16)
    dtv_ref[...] = tb[text // 8:].astype(F32).reshape(text, width).astype(BF16)
    fold_cols(2)
    fold_cols(3)


def hand_on(*refs):
    count = (len(refs) - 1) // 2
    copies = []
    for n in range(count):
        c = pltpu.make_async_copy(refs[n], refs[count + n], refs[-1].at[n])
        c.start()
        copies.append(c)
    for c in copies:
        c.wait()


def solution(mesh):
    n_ha, n_wa = mesh.shape["ha"], mesh.shape["wa"]

    def local(queries, keys, values, out_grad, log_norm, delta_rows, text_keys, text_values, window_table):
        frames, tile, _, width = queries.shape
        heads = width // HDIM
        text = text_keys.shape[0]
        plane = tile * tile
        cells = frames * plane
        part = width // GROUPS
        bands = tile // HALO
        band = frames * HALO * HALO
        strip = bands * band
        rim = frames * HALO * tile
        plan = text_plan(n_ha, n_wa, 2 * text // 8, width)
        most = max([far - 1 if how == "direct" else 1 for _, far, _, _, how in plan] + [1])
        received = []
        for stage_of in plan:
            _, far, rows, wide, how = stage_of
            n = far - 1 if how == "direct" else 1
            if coded(stage_of):
                received += [pltpu.VMEM((n, rows * 8, wide), I16), pltpu.VMEM((n, 1, HDIM), F32)] * 2
            else:
                received.append(pltpu.VMEM((n, rows, 8, wide), F32))
        sem = pltpu.SemaphoreType.DMA
        anywhere = pl.BlockSpec(memory_space=pltpu.HBM)
        vmem = pl.BlockSpec(memory_space=pltpu.VMEM)
        rows = frames * plane
        results = pl.pallas_call(
            functools.partial(kernel, n_ha, n_wa, plan),
            out_shape=[pltpu.VMEM((rows, width), BF16)] * 3 + [pltpu.VMEM((text, width), BF16)] * 2,
            in_specs=[anywhere] * 9,
            out_specs=[vmem] * 5,
            scratch_shapes=[
                pltpu.SMEM(window_table.shape, jnp.int32),
                *[pltpu.VMEM((frames, plane, width), BF16)] * 4,
                *[pltpu.VMEM((cells, heads), F32)] * 2,
                *[pltpu.VMEM((text, width), BF16)] * 2,
                pltpu.VMEM((GROUPS, 2, 2, strip, part), BF16),
                pltpu.VMEM((GROUPS, 2, 2, strip, part), BF16),
                pltpu.VMEM((GROUPS, 2, 2, frames, HALO * tile, part), BF16),
                pltpu.VMEM((GROUPS, 2, 4 * band, part), BF16),
                pltpu.VMEM((GROUPS, 2, 2, strip, part), F32),
                pltpu.VMEM((GROUPS, 2, 2, strip, part), I16),
                pltpu.VMEM((GROUPS, 2, 2, rim, part), I16),
                pltpu.VMEM((GROUPS, 2, 2, 2 * band, part), I16),
                pltpu.VMEM((GROUPS, 2, 2, strip, part), I16),
                pltpu.VMEM((GROUPS, 2, 2, rim, part), I16),
                pltpu.VMEM((GROUPS, 2, 2, 2 * band, part), I16),
                pltpu.VMEM((GROUPS, 2, 2, 2, HDIM), F32),
                pltpu.VMEM((GROUPS, 2, 2, part), F32),
                pltpu.VMEM((GROUPS, 2, 2, part), F32),
                pltpu.VMEM((GROUPS, 2, 2, 2, HDIM), F32),
                pltpu.VMEM((GROUPS, 2, 2, part), F32),
                pltpu.VMEM((GROUPS, 2, 2, part), F32),
                pltpu.VMEM((2, cells, width), F32),
                pltpu.VMEM((cells, width), F32),
                pltpu.VMEM((2 * rim + 4 * band + 2 * strip, cells), F32),
                pltpu.VMEM((heads, cells), F32),
                pltpu.VMEM((heads, cells), F32),
                pltpu.VMEM((2 * text // 8, 8, width), F32),
                pltpu.VMEM((2 * text // 8, 8, width), BF16),
                *received,
                sem((9,)),
                sem((GROUPS, 2, 2)), sem((GROUPS, 2, 2)),
                sem((GROUPS, 2, 2)), sem((GROUPS, 2, 2)),
                sem((GROUPS, 2, 2)), sem((GROUPS, 2, 2)),
                sem((GROUPS, 2, 2, 2)), sem((GROUPS, 2, 2, 2)),
                sem((GROUPS, 2, 2)), sem((GROUPS, 2, 2)),
                sem((GROUPS, 2, 2)), sem((GROUPS, 2, 2)),
                sem((len(plan), most, 2)), sem((len(plan), most, 2)),
                sem((len(plan), most)), sem((len(plan), most)),
            ],
            compiler_params=pltpu.CompilerParams(
                collective_id=0, has_side_effects=True, vmem_limit_bytes=32 * 1024 * 1024
            ),
        )(*(
            pltpu.with_memory_space_constraint(x, pltpu.HBM) for x in (
                window_table,
                *(x.reshape(frames, plane, width) for x in (queries, keys, values, out_grad)),
                *(x.transpose(1, 2, 3, 0).reshape(cells, heads) for x in (log_norm, delta_rows)),
                text_keys, text_values,
            )
        ))

        dq, dk, dv, dtk, dtv = pl.pallas_call(
            hand_on,
            out_shape=[jax.ShapeDtypeStruct((rows, width), BF16)] * 3 + [jax.ShapeDtypeStruct((text, width), BF16)] * 2,
            in_specs=[vmem] * 5,
            out_specs=[anywhere] * 5,
            scratch_shapes=[sem((5,))],
            compiler_params=pltpu.CompilerParams(vmem_limit_bytes=4 * 1024 * 1024),
        )(*(pltpu.with_memory_space_constraint(x, pltpu.VMEM) for x in results))
        return *(x.reshape(queries.shape) for x in (dq, dk, dv)), dtk, dtv

    tile_spec = P("group", "ha", "wa", None)
    stat_spec = P(None, "group", "ha", "wa")
    text_spec = P("group", None)
    return jax.shard_map(
        local,
        mesh=mesh,
        in_specs=(tile_spec,) * 4 + (stat_spec,) * 2 + (text_spec,) * 2 + (P(),),
        out_specs=(tile_spec,) * 3 + (text_spec,) * 2,
        check_vma=False,
    )
```
